128 devices in a mesh: grp: 2 (over core), ta: 4 (over y), ha: 2 (over z_lo), wa: 8 (over x, z_hi).
Axes of the slice: x: 4, y: 4, z: 4 (z_hi: 2, z_lo: 2; z = z_hi * 2 + z_lo), core: 2. Of those that a mesh axis runs over, the one named last changes fastest.
Arguments:
- query_tiles: bfloat16 [4, 2, 8, 256, 3072], P('ta', 'ha', 'wa', None, 'grp'), may hold values from -11 to 11
- key_tiles: bfloat16 [4, 2, 8, 256, 3072], P('ta', 'ha', 'wa', None, 'grp'), may hold values from -11 to 11
- value_tiles: bfloat16 [4, 2, 8, 256, 3072], P('ta', 'ha', 'wa', None, 'grp'), may hold values from -6 to 6
- out_weight: bfloat16 [3072, 3072], P('grp'), may hold values from -0.15625 to 0.15625
- gate: bfloat16 [3072], P('grp'), may hold values from 8 to 64
Outputs:
- branch: bfloat16 [4, 2, 8, 256, 3072], P('ta', 'ha', 'wa', None, 'grp')
The draws below stay inside these ranges and needn't reach their ends.
All inputs are finite; a program needn't handle non-finite values.
Results may differ from the reference program's by a relative error of at most 0.0057.
Values may be sent and summed in bfloat16 or wider, within the bound.
No kernel may reach another device: no remote copies, remote signals or barrier semaphores. Data moves between devices by JAX's collectives and lax.ppermute only.
A program may use at most 256 MiB of HBM per device.

```python
import math
import jax
import jax.numpy as jnp
from jax import lax

D = 3072
HEADS = 24
HD = 128
TOK = 256
N_TA = 4
N_HA = 2
N_WA = 8


def drawn_pair(key):
    base = jax.random.fold_in(key, 11)
    first, second = jax.random.split(base, 2)
    features = HEADS * HD
    shape = (N_TA * N_HA * N_WA * TOK, features)
    queries = jnp.clip(jax.random.normal(first, shape, jnp.float32), -4.0, 4.0)
    keys_drawn = jnp.clip(jax.random.normal(second, shape, jnp.float32), -4.0, 4.0)
    full = (N_TA, N_HA, N_WA, TOK, features)
    return (queries.reshape(full).astype(jnp.bfloat16), keys_drawn.reshape(full).astype(jnp.bfloat16))


def draw_query_tiles(key, part):
    return drawn_pair(key)[0]


def draw_key_tiles(key, part):
    return drawn_pair(key)[1]


def raised(values, rng, source, target, shards_of, factor):
    owner, partner = [(jnp.arange(values.shape[axis_at]) // (values.shape[axis_at] // shards_of)).reshape([-1 if axis == axis_at else 1 for axis in range(values.ndim)]) for axis_at in (source, target)]
    chosen = jax.random.permutation(rng, shards_of)[partner]
    strong = (owner == chosen) | (owner == (partner + shards_of // 2) % shards_of)
    return jnp.where(strong, factor * values, values)


def levels(own_key, extent, shards, least, top_value):
    factor_of, own = 1.0, jax.random.fold_in(own_key, 6)
    for position, parts in shards:
        draws = jnp.exp(jax.random.uniform(jax.random.fold_in(own, position), (parts,), jnp.float32, least / len(shards), top_value / len(shards)))
        factor_of = factor_of * jnp.repeat(draws, extent[position] // parts).reshape([-1 if axis == position else 1 for axis in range(len(extent))])
    return factor_of


def noise(stream_key, dims, scale, reach, cuts=(), held_as=jnp.bfloat16):
    drawn = scale * jax.random.normal(stream_key, dims, jnp.float32)
    if cuts:
        drawn = drawn * levels(stream_key, dims, cuts, -0.22, 0.18)
    return jnp.clip(drawn, -reach, reach).astype(held_as)


def heavy_noise(stream_key, extent, spread, bound, cuts, heavy, kind=jnp.bfloat16):
    values = spread * jax.random.normal(stream_key, extent, jnp.float32)
    if cuts:
        values = values * levels(stream_key, extent, cuts, -0.22, 0.18)
    return jnp.clip(raised(values, jax.random.fold_in(stream_key, 3), *heavy), -bound, bound).astype(kind)


def setup_inputs(seed: int = 0) -> dict:
    splits = jax.random.split(jax.random.key(seed), 6)
    return {
        "query_tiles": draw_query_tiles(jax.random.fold_in(splits[5], 71), 0),
        "key_tiles": draw_key_tiles(jax.random.fold_in(splits[5], 71), 0),
        "value_tiles": noise(splits[2], (N_TA, N_HA, N_WA, TOK, HEADS * HD), 1.0, 6.0, ((0, 4), (1, 2), (2, 8), (4, 2))),
        "out_weight": heavy_noise(splits[3], (HEADS * HD, D), (HEADS * HD) ** -0.5, 0.15625, ((0, 2),), (0, 1, 2, 2.0)),
        "gate": jnp.clip(jnp.exp(math.log(64.0) - 2.0794415 * jax.random.uniform(splits[4], (D,), jnp.float32) ** levels(splits[4], (D,), ((0, 2),), -0.2, 0.2)), 8.0, 64.0).astype(jnp.bfloat16),
    }


def reference(query_tiles, key_tiles, value_tiles, out_weight, gate):
    features = HEADS * HD
    margin = ((1, 1), (1, 1), (1, 1), (0, 0), (0, 0))
    keys_padded = jnp.pad(key_tiles, margin)
    values_padded = jnp.pad(value_tiles, margin)
    present = jnp.pad(jnp.ones((N_TA, N_HA, N_WA), jnp.int32), 1)

    def one_block(flat):
        time_index = (flat // (N_HA * N_WA)).astype(jnp.int32)
        height_index = ((flat // N_WA) % N_HA).astype(jnp.int32)
        width_index = (flat % N_WA).astype(jnp.int32)
        zero = jnp.zeros((), jnp.int32)
        starts = (time_index, height_index, width_index, zero, zero)
        queries = lax.dynamic_slice(query_tiles, starts, (1, 1, 1, TOK, features))
        queries = queries.reshape(TOK, HEADS, HD).astype(jnp.float32)
        near_keys = lax.dynamic_slice(keys_padded, starts, (3, 3, 3, TOK, features))
        near_keys = near_keys.reshape(27 * TOK, HEADS, HD).astype(jnp.float32)
        near_values = lax.dynamic_slice(values_padded, starts, (3, 3, 3, TOK, features))
        near_values = near_values.reshape(27 * TOK, HEADS, HD).astype(jnp.float32)
        live = lax.dynamic_slice(present, (time_index, height_index, width_index), (3, 3, 3)).reshape(27)
        live_keys = jnp.repeat(live, TOK) > 0
        scores = jnp.einsum("qhd,khd->hqk", queries, near_keys) * (HD ** -0.5)
        scores = jnp.where(live_keys[None, None, :], scores, -1e30)
        peak = jnp.max(scores, axis=-1, keepdims=True)
        expo = jnp.exp(scores - peak)
        totals = jnp.sum(expo, axis=-1)
        probs = lax.optimization_barrier(expo.astype(jnp.bfloat16)).astype(jnp.float32)
        mixed = jnp.einsum("hqk,khd->qhd", probs, near_values) / jnp.transpose(totals)[:, :, None]
        attended = mixed.astype(jnp.bfloat16).reshape(TOK, features)
        projected = jnp.dot(attended, out_weight, preferred_element_type=jnp.float32)
        return (gate.astype(jnp.float32) * projected).astype(jnp.bfloat16)

    result = lax.map(one_block, jnp.arange(N_TA * N_HA * N_WA, dtype=jnp.int32))
    return result.reshape(N_TA, N_HA, N_WA, TOK, D)
```

```python
import functools
import math

import jax
import jax.numpy as jnp
from jax import lax
from jax.experimental import pallas as pl
from jax.experimental.pallas import tpu as pltpu
from jax.sharding import PartitionSpec as P

HD = 128
TILE = 256
AXES = ("grp", "ta", "ha", "wa")
FLIP = (0, 1, 1, 0)
SPLITS = ((0, 1, 2),)
SCALE = HD**-0.5 * math.log2(math.e)
F32 = jnp.float32
BF16 = jnp.bfloat16


def flat(core, y, z, x):
    return ((core * 4 + y) * 2 + z % 2) * 8 + x * 2 + z // 2


def pairs(move):
    found = []
    for core in range(2):
        for y in range(4):
            for z in range(4):
                for x in range(4):
                    there = move(core, y, z, x)
                    if there is not None:
                        found.append((flat(core, y, z, x), flat(*there)))
    return sorted(found)


def out_to_heads(step):
    def move(core, y, z, x):
        half = y // 2
        return FLIP[y], (core if half == 0 else 3 - core), (z + step) % 4, x

    return pairs(move)


def back_to_tiles(step):
    return sorted((b, a) for a, b in out_to_heads(step))


def to_partner(core, y, z, x):
    return 1 - core, y, z, x


def to_outer(core, y, z, x):
    return (core, 3 - y, z, x) if core == 1 else None


def to_edge(step):
    def move(core, y, z, x):
        x_there = x + 1 if ((z - step) % 4) >= 2 else x - 1
        return (core, y, z, x_there) if 0 <= x_there < 4 else None

    return pairs(move)


def send(x, perm):
    return lax.ppermute(x, AXES, perm)


def pack_body(place, *refs):
    ins, outs = refs[:12], refs[12:]
    at = 0
    for group in SPLITS:
        for step in range(4):
            q_in, k_in, v_in = ins[3 * step : 3 * step + 3]
            kv_out, q_out = outs[at : at + 2]
            at += 2
            for n, head in enumerate(group):
                cols = slice(head * HD, (head + 1) * HD)
                kv_out[n, 0] = k_in[:, cols]
                kv_out[n, 1] = v_in[:, cols]
                q_out[n] = q_in[:, cols]


def pack(place, q, k, v):
    specs = []
    for step in range(4):
        spec = pl.BlockSpec((TILE, 3 * HD), lambda i, place, step=step: (0, (place[0] + step) % 4))
        specs += [spec] * 3
    shapes, out_specs = [], []
    for group in SPLITS:
        for step in range(4):
            for dims in ((len(group), 2, TILE, HD), (len(group), TILE, HD)):
                shapes.append(jax.ShapeDtypeStruct(dims, BF16))
                out_specs.append(pl.BlockSpec(dims, lambda i, place, r=len(dims): (0,) * r))
    flat_out = pl.pallas_call(
        pack_body,
        grid_spec=pltpu.PrefetchScalarGridSpec(
            num_scalar_prefetch=1, grid=(1,), in_specs=specs, out_specs=out_specs
        ),
        out_shape=shapes,
        name="pack",
    )(place, *([q, k, v] * 4))
    return [
        [(flat_out[2 * (4 * g + step)], flat_out[2 * (4 * g + step) + 1]) for step in range(4)]
        for g in range(len(SPLITS))
    ]


def attend_body(count, place, *refs):
    kv_in, refs = refs[:24], refs[24:]
    q_in, refs = refs[:4], refs[4:]
    outs, refs = refs[:4], refs[4:]
    kv_held, q_held, q_raw, peak, mixed, arrived = refs
    z, core, x = place[0], place[1], place[2]
    has_outer = core == 1

    def copies(head):
        kv = [
            pltpu.make_async_copy(kv_in[t].at[head], kv_held.at[t], arrived.at[t])
            for t in range(24)
        ]
        return kv

    ones = jnp.ones((TILE, HD), BF16)

    def update(side, tiles):
        q = q_held[side]
        keys = jnp.concatenate([kv_held[t, 0] for t in tiles], axis=0)
        values = jnp.concatenate(
            [jnp.concatenate([kv_held[t, 1], ones], axis=1) for t in tiles], axis=0
        )
        scores = lax.dot_general(q, keys, (((1,), (1,)), ((), ())), preferred_element_type=F32)
        scores = scores * SCALE
        before = peak[side]
        now = jnp.maximum(before, jnp.max(scores, axis=1, keepdims=True))
        peak[side] = now
        shrink = jnp.exp2(before - now)
        probs = jnp.exp2(scores - jnp.tile(now, (1, len(tiles) * TILE // HD)))
        fresh = jnp.dot(probs.astype(BF16), values, preferred_element_type=F32)
        mixed[side] = mixed[side] * jnp.concatenate([shrink, shrink], axis=1) + fresh

    for head in range(count):
        kv = copies(head)
        for c in kv:
            c.start()
        for step in range(4):
            z_from = (z - step + 4) % 4
            q_held[z_from // 2, pl.ds(pl.multiple_of((z_from % 2) * TILE, TILE), TILE), :] = q_in[
                step
            ][head]
        peak[...] = jnp.full_like(peak, -1e30)
        mixed[...] = jnp.zeros_like(mixed)
        for c in kv:
            c.wait()

        def main(side, carry):
            update(side, (0, 1, 2, 3))
            update(side, (4, 5, 6, 7))

            @pl.when(has_outer)
            def _():
                update(side, (8, 9, 10, 11))

            return carry

        lax.fori_loop(0, 2, main, 0)

        def edges(step, carry):
            z_from = (z - step + 4) % 4
            side = 1 - z_from // 2
            live = jnp.where(side == 0, x > 0, x < 3)

            @pl.when(live)
            def _():
                update(side, (12 + step, 16 + step))

                @pl.when(has_outer)
                def _():
                    update(side, (20 + step,))

            return carry

        lax.fori_loop(0, 4, edges, 0)

        for step in range(4):
            z_from = (z - step + 4) % 4
            rows = pl.ds(pl.multiple_of((z_from % 2) * TILE, TILE), TILE)
            total = mixed[z_from // 2, rows, HD:]
            outs[step][:, head * HD : (head + 1) * HD] = (
                mixed[z_from // 2, rows, :HD] / total
            ).astype(BF16)


def attend(place, count, tiles, queries):
    hbm = pl.BlockSpec(memory_space=pltpu.MemorySpace.HBM)
    whole = pl.BlockSpec(memory_space=pltpu.MemorySpace.VMEM)
    smem = pl.BlockSpec(memory_space=pltpu.MemorySpace.SMEM)
    keys_seen = 18 * TILE
    return pl.pallas_call(
        functools.partial(attend_body, count),
        in_specs=[smem] + [hbm] * 24 + [whole] * 4,
        out_specs=[whole] * 4,
        out_shape=[jax.ShapeDtypeStruct((TILE, count * HD), BF16)] * 4,
        scratch_shapes=[
            pltpu.VMEM((24, 2, TILE, HD), BF16),
            pltpu.VMEM((2, 2 * TILE, HD), BF16),
            pltpu.VMEM((4, TILE, HD), BF16),
            pltpu.VMEM((2, 2 * TILE, HD), F32),
            pltpu.VMEM((2, 2 * TILE, 2 * HD), F32),
            pltpu.SemaphoreType.DMA((24,)),
        ],
        cost_estimate=pl.CostEstimate(
            flops=count * 4 * 1024 * keys_seen * HD,
            bytes_accessed=count * 24 * 2 * TILE * HD * 2,
            transcendentals=count * 1024 * keys_seen,
        ),
        compiler_params=pltpu.CompilerParams(vmem_limit_bytes=48 * 1024 * 1024),
        name="attend",
    )(place, *tiles, *queries)


def project_body(groups, place, *refs):
    own, refs = refs[: 4 * groups], refs[4 * groups :]
    other, refs = refs[: 4 * groups], refs[4 * groups :]
    w_own, w_other, gate, out = refs
    z = place[0]
    total = None
    for chunks, weight in ((own, w_own), (other, w_other)):
        for step in range(4):
            rows = pl.ds(pl.multiple_of(((z + step) % 4) * 3 * HD, 3 * HD), 3 * HD)
            left = jnp.concatenate([chunks[4 * g + step][...] for g in range(groups)], axis=1)
            term = jnp.dot(left, weight[rows, :], preferred_element_type=F32)
            total = term if total is None else total + term
    out[...] = (gate[...].astype(F32) * total).astype(BF16)


def project(place, own, other, weight, weight_other, gate):
    groups = len(own) // 4
    features = weight.shape[0]
    cols = features // 3
    chunk = [pl.BlockSpec(a.shape, lambda i, place: (0, 0)) for a in own]
    return pl.pallas_call(
        functools.partial(project_body, groups),
        grid_spec=pltpu.PrefetchScalarGridSpec(
            num_scalar_prefetch=1,
            grid=(3,),
            in_specs=chunk
            + chunk
            + [
                pl.BlockSpec((features, cols), lambda i, place: (0, place[1] * 3 + i)),
                pl.BlockSpec((features, cols), lambda i, place: (0, i)),
                pl.BlockSpec((1, cols), lambda i, place: (0, i)),
            ],
            out_specs=pl.BlockSpec((TILE, cols), lambda i, place: (0, i)),
        ),
        out_shape=jax.ShapeDtypeStruct((TILE, features), BF16),
        cost_estimate=pl.CostEstimate(
            flops=2 * TILE * 2 * features * features,
            bytes_accessed=4 * features * features,
            transcendentals=0,
        ),
        compiler_params=pltpu.CompilerParams(vmem_limit_bytes=48 * 1024 * 1024),
        name="project",
    )(place, *own, *other, weight, weight_other, gate)


def shards(query_tiles, key_tiles, value_tiles, out_weight, gate):
    features = query_tiles.shape[4]
    q, k, v = (a.reshape(TILE, features) for a in (query_tiles, key_tiles, value_tiles))
    core, y = lax.axis_index("grp"), lax.axis_index("ta")
    wide = lax.axis_index("wa")
    z, x = (wide % 2) * 2 + lax.axis_index("ha"), wide // 2
    place = jnp.stack([z, core, x, y]).astype(jnp.int32)
    partner = pairs(to_partner)
    outer = pairs(to_outer)
    weight_away = lax.dynamic_slice_in_dim(out_weight, (1 - core) * features, features, axis=1)
    weight_other = send(weight_away, partner)
    packed = pack(place, q, k, v)
    attended, attended_other = [], []
    for group, blocks in zip(SPLITS, packed):
        kv_own = [send(blocks[s][0], out_to_heads(s)) for s in range(4)]
        queries = [send(blocks[s][1], out_to_heads(s)) for s in range(4)]
        kv_outer = [send(a, outer) for a in kv_own]
        edge_own = [send(kv_own[s], to_edge(s)) for s in range(4)]
        kv_inner = [send(a, partner) for a in kv_own]
        edge_outer = [send(kv_outer[s], to_edge(s)) for s in range(4)]
        edge_inner = [send(a, partner) for a in edge_own]
        tiles = kv_own + kv_inner + kv_outer + edge_own + edge_inner + edge_outer
        outs = attend(place, len(group), tiles, queries)
        outs = [send(outs[s], back_to_tiles(s)) for s in range(4)]
        attended += outs
        attended_other += [send(a, partner) for a in outs]
    branch = project(place, attended, attended_other, out_weight, weight_other, gate.reshape(1, -1))
    return branch.reshape(1, 1, 1, TILE, features)


def solution(mesh):
    spec = P("ta", "ha", "wa", None, "grp")
    return jax.shard_map(
        shards,
        mesh=mesh,
        in_specs=(spec, spec, spec, P("grp", None), P("grp")),
        out_specs=spec,
        check_vma=False,
    )
```

```python
import functools
import math

import jax
import jax.numpy as jnp
from jax import lax
from jax.experimental import pallas as pl
from jax.experimental.pallas import tpu as pltpu
from jax.sharding import PartitionSpec as P


HD = 128
TILE = 256
AXES = ("grp", "ta", "ha", "wa")
FLIP = (0, 1, 1, 0)
HEADS = 3
ROWS = 144
LIMIT = 2.0**100
SCALE = HD**-0.5 * math.log2(math.e)
F32 = jnp.float32
BF16 = jnp.bfloat16


def flat(core, y, z, x):
    return ((core * 4 + y) * 2 + z % 2) * 8 + x * 2 + z // 2


def pairs(move):
    found = []
    for core in range(2):
        for y in range(4):
            for z in range(4):
                for x in range(4):
                    there = move(core, y, z, x)
                    if there is not None:
                        found.append((flat(core, y, z, x), flat(*there)))
    return sorted(found)


def out_to_heads(step):
    def move(core, y, z, x):
        half = y // 2
        return FLIP[y], (core if half == 0 else 3 - core), (z + step) % 4, x

    return pairs(move)


def back_to_tiles(step):
    return sorted((b, a) for a, b in out_to_heads(step))


def to_partner(core, y, z, x):
    return 1 - core, y, z, x


def to_outer(core, y, z, x):
    return (core, 3 - y, z, x) if core == 1 else None


def send(x, perm):
    return lax.ppermute(x, AXES, perm)


def turned(block):
    across = block.T
    return across[:, :HD], across[:, HD:]


def pack_body(place, *refs):
    ins, outs = refs[:12], refs[12:]
    for step in range(4):
        q_in, k_in, v_in = ins[3 * step : 3 * step + 3]
        kv_out, q_out = outs[2 * step : 2 * step + 2]
        for head in range(HEADS):
            cols = slice(head * HD, (head + 1) * HD)
            kv_out[head, 0] = k_in[:, cols]
            kv_out[head, 1, :HD], kv_out[head, 1, HD:] = turned(v_in[:, cols])
            q_out[head, :HD], q_out[head, HD:] = turned(q_in[:, cols])


def pack(place, q, k, v):
    specs, shapes, out_specs = [], [], []
    for step in range(4):
        spec = pl.BlockSpec((TILE, 3 * HD), lambda i, place, step=step: (0, (place[0] + step) % 4))
        specs += [spec] * 3
        for dims in ((HEADS, 2, TILE, HD), (HEADS, TILE, HD)):
            shapes.append(jax.ShapeDtypeStruct(dims, BF16))
            out_specs.append(pl.BlockSpec(dims, lambda i, place, r=len(dims): (0,) * r))
    flat_out = pl.pallas_call(
        pack_body,
        grid_spec=pltpu.PrefetchScalarGridSpec(
            num_scalar_prefetch=1, grid=(1,), in_specs=specs, out_specs=out_specs
        ),
        out_shape=shapes,
        name="pack",
    )(place, *([q, k, v] * 4))
    return flat_out[0::2], flat_out[1::2]


VMEM = pl.BlockSpec(memory_space=pltpu.MemorySpace.VMEM)
SMEM = pl.BlockSpec(memory_space=pltpu.MemorySpace.SMEM)


def local_call(body, place, operands, shapes, flops=0, limit=24, aliases=None):
    single = not isinstance(shapes, (list, tuple))
    listed = [shapes] if single else list(shapes)
    moved = sum(math.prod(a.shape) * a.dtype.itemsize for a in list(operands) + listed)
    return pl.pallas_call(
        body,
        in_specs=[SMEM] + [VMEM] * len(operands),
        out_specs=VMEM if single else [VMEM] * len(listed),
        out_shape=shapes,
        cost_estimate=pl.CostEstimate(flops=flops, bytes_accessed=moved, transcendentals=0),
        compiler_params=pltpu.CompilerParams(vmem_limit_bytes=limit * 1024 * 1024),
        input_output_aliases=aliases or {},
    )(place, *operands)


def gather_body(place, *refs):
    chunks, outs = refs[:4], refs[4:]
    for step in range(4):
        z_from = (place[0] - step + 4) % 4
        for high in range(2):

            @pl.when(z_from // 2 == high)
            def _():
                outs[high][:, z_from % 2] = chunks[step][...]


def gather(place, chunks):
    shape = jax.ShapeDtypeStruct((HEADS, 2, 2, TILE, HD), BF16)
    return local_call(gather_body, place, chunks, [shape] * 2)


MIXED = jax.ShapeDtypeStruct((HEADS, 2, ROWS, 2 * TILE), F32)
PEAK = jax.ShapeDtypeStruct((HEADS, 2, 1, 2 * TILE), F32)
TURNED = jax.ShapeDtypeStruct((HEADS, 4, 2 * HD, TILE), BF16)


def spread(place, q_in, turned_q):
    for step in range(4):
        z_from = (place[0] - step + 4) % 4
        for head in range(HEADS):
            both = jnp.concatenate([q_in[step][head, :HD], q_in[step][head, HD:]], axis=1)
            scaled = both.astype(F32) * SCALE
            high = scaled.astype(BF16)
            turned_q[head, z_from, :HD] = high
            turned_q[head, z_from, HD:] = (scaled - high.astype(F32)).astype(BF16)


def loaded(tiles):
    keys = jnp.concatenate([ref[head, low, 0] for ref, head, low in tiles], axis=0)
    values = jnp.concatenate(
        [
            ref[head, low, 1, half * HD : (half + 1) * HD]
            for ref, head, low in tiles
            for half in range(2)
        ],
        axis=1,
    )
    return keys, jnp.concatenate([values, jnp.ones((ROWS - HD, values.shape[1]), BF16)], axis=0)


def queries_of(turned_q, head, side):
    return jnp.concatenate([turned_q[head, 2 * side], turned_q[head, 2 * side + 1]], axis=1)


def scored(keys, queries):
    return jnp.dot(jnp.concatenate([keys, keys], axis=1), queries, preferred_element_type=F32)


def quick(queries, tiles, level, bias=None):
    keys, values = loaded(tiles)
    scores = scored(keys, queries) - (level if bias is None else level - bias)
    return jnp.dot(values, jnp.exp2(scores).astype(BF16), preferred_element_type=F32)


def careful(turned_q, mixed, peak, head, side, ref, bias=0.0):
    def one(low, carry):
        keys, values = loaded([(ref, head, low)])
        scores = scored(keys, queries_of(turned_q, head, side)) + bias
        before = peak[head, side]
        top = jnp.maximum(before, jnp.max(scores, axis=0, keepdims=True))
        probs = jnp.exp2(scores - top).astype(BF16)
        fresh = jnp.dot(values, probs, preferred_element_type=F32)
        mixed[head, side] = mixed[head, side] * jnp.exp2(before - top) + fresh
        peak[head, side] = top
        return carry

    lax.fori_loop(0, 2, one, 0)


def both_lows(head, *refs):
    return [(ref, head, low) for ref in refs for low in range(2)]


def within(sums):
    return jnp.max(sums) < LIMIT


def first_body(place, *refs):
    own, inner, q_in, (turned_q, mixed, peak) = refs[:2], refs[2:4], refs[4:8], refs[8:]
    spread(place, q_in, turned_q)

    def one(head, carry):
        fresh = []
        for side in range(2):
            queries = queries_of(turned_q, head, side)
            level = jnp.max(scored(own[0][head, 0, 0, :HD], queries), axis=0, keepdims=True)
            peak[head, side] = level
            fresh.append(
                quick(queries, both_lows(head, *own), level)
                + quick(queries, both_lows(head, *inner), level)
            )
        good = within(jnp.maximum(fresh[0][HD : HD + 1], fresh[1][HD : HD + 1]))

        @pl.when(good)
        def _():
            mixed[head, 0], mixed[head, 1] = fresh

        @pl.when(jnp.logical_not(good))
        def _():
            def redo(side, carry):
                mixed[head, side] = jnp.zeros((ROWS, 2 * TILE), F32)
                for ref in (*own, *inner):
                    careful(turned_q, mixed, peak, head, side, ref)
                return carry

            lax.fori_loop(0, 2, redo, 0)

        return carry

    lax.fori_loop(0, HEADS, one, 0)


def more(turned_q, mixed, peak, head, shares, biases=(None, None)):
    fresh = []
    for side in range(2):
        queries = queries_of(turned_q, head, side)
        fresh.append(
            mixed[head, side]
            + quick(queries, both_lows(head, *shares[side]), peak[head, side], biases[side])
        )
    good = within(jnp.maximum(fresh[0][HD : HD + 1], fresh[1][HD : HD + 1]))

    @pl.when(good)
    def _():
        mixed[head, 0], mixed[head, 1] = fresh

    @pl.when(jnp.logical_not(good))
    def _():
        for side in range(2):
            for ref in shares[side]:
                careful(
                    turned_q, mixed, peak, head, side, ref, 0.0 if biases[side] is None else biases[side]
                )


def edge_biases(place):
    return [jnp.where(place[2] == end, -1e30, 0.0).astype(F32) for end in (0, 3)]


def second_body(place, *refs):
    outer, (turned_q, _, _, mixed, peak) = refs[:2], refs[2:]

    @pl.when(place[1] == 1)
    def _():
        def one(head, carry):
            more(turned_q, mixed, peak, head, (outer, outer))
            return carry

        lax.fori_loop(0, HEADS, one, 0)


def third_body(place, *refs):
    left, right, (turned_q, _, _, mixed, peak) = refs[:2], refs[2:4], refs[4:]
    biases = edge_biases(place)

    def one(head, carry):
        more(turned_q, mixed, peak, head, (left, right), biases)
        return carry

    lax.fori_loop(0, HEADS, one, 0)


def last_body(place, *refs):
    left, right, turned_q, mixed_in, peak_in = refs[:5]
    outs, (done, mixed, peak) = refs[5:9], refs[9:]
    biases = edge_biases(place)
    mixed[...] = mixed_in[...]
    peak[...] = peak_in[...]

    @pl.when(place[1] == 1)
    def _():
        def one(head, carry):
            more(turned_q, mixed, peak, head, ((left,), (right,)), biases)
            return carry

        lax.fori_loop(0, HEADS, one, 0)

    def finish(head, carry):
        for side in range(2):
            total = mixed[head, side, HD : HD + 1]
            result = (mixed[head, side, :HD] / total).astype(BF16).T
            for low in range(2):
                done[2 * side + low, head] = result[low * TILE : (low + 1) * TILE]
        return carry

    lax.fori_loop(0, HEADS, finish, 0)

    for step in range(4):
        z_from = (place[0] - step + 4) % 4
        for head in range(HEADS):
            outs[step][:, head * HD : (head + 1) * HD] = done[z_from, head]


def last(place, operands, flops):
    out = jax.ShapeDtypeStruct((TILE, HEADS * HD), BF16)
    return pl.pallas_call(
        last_body,
        in_specs=[SMEM] + [VMEM] * len(operands),
        out_specs=[VMEM] * 4,
        out_shape=[out] * 4,
        scratch_shapes=[
            pltpu.VMEM((4, HEADS, TILE, HD), BF16),
            pltpu.VMEM(MIXED.shape, F32),
            pltpu.VMEM(PEAK.shape, F32),
        ],
        cost_estimate=pl.CostEstimate(flops=flops, bytes_accessed=1 << 20, transcendentals=0),
        compiler_params=pltpu.CompilerParams(vmem_limit_bytes=24 * 1024 * 1024),
        name="last",
    )(place, *operands)


def terms_body(mine, place, *refs):
    chunks, weight, out, joined = refs[:4], refs[4], refs[5], refs[6]
    width = out.shape[1]
    side = place[1] if mine else 1 - place[1]
    for step in range(4):
        slot = (place[0] + step) % 4
        for head in range(HEADS):
            joined[:, pl.ds(pl.multiple_of((slot * HEADS + head) * HD, HD), HD)] = chunks[step][
                :, head * HD : (head + 1) * HD
            ]
    cols = pl.ds(pl.multiple_of(side * width, width), width)
    out[...] = jnp.dot(joined[...], weight[:, cols], preferred_element_type=F32)


def terms(place, chunks, weight, mine):
    features = weight.shape[0]
    return pl.pallas_call(
        functools.partial(terms_body, mine),
        in_specs=[SMEM] + [VMEM] * 5,
        out_specs=VMEM,
        out_shape=jax.ShapeDtypeStruct((TILE, features), F32),
        scratch_shapes=[pltpu.VMEM((TILE, features), BF16)],
        cost_estimate=pl.CostEstimate(
            flops=2 * TILE * features * features, bytes_accessed=1 << 20, transcendentals=0
        ),
        compiler_params=pltpu.CompilerParams(vmem_limit_bytes=24 * 1024 * 1024),
        name="home" if mine else "away",
    )(place, *chunks, weight)


def close_body(place, here, arrived, gate, out):
    out[...] = (gate[...].astype(F32) * (here[...] + arrived[...])).astype(BF16)


def shards(query_tiles, key_tiles, value_tiles, out_weight, gate):
    features = query_tiles.shape[4]
    q, k, v = (a.reshape(TILE, features) for a in (query_tiles, key_tiles, value_tiles))
    core, y = lax.axis_index("grp"), lax.axis_index("ta")
    wide = lax.axis_index("wa")
    z, x = (wide % 2) * 2 + lax.axis_index("ha"), wide // 2
    place = jnp.stack([z, core, x, y]).astype(jnp.int32)
    partner, outer_pairs = pairs(to_partner), pairs(to_outer)
    to_right = pairs(lambda core, y, z, x: (core, y, z, x + 1) if x < 3 else None)
    to_left = pairs(lambda core, y, z, x: (core, y, z, x - 1) if x > 0 else None)
    flops_of = lambda tiles: HEADS * 4 * TILE * tiles * TILE * 6 * HD

    kv_sent, q_sent = pack(place, q, k, v)
    kv = [send(kv_sent[s], out_to_heads(s)) for s in range(4)]
    queries = [send(q_sent[s], out_to_heads(s)) for s in range(4)]
    own = gather(place, kv)
    outer = [send(own[i], outer_pairs) for i in range(2)]
    inner = [send(own[i], partner) for i in range(2)]
    right, left = send(own[0], to_left), send(own[1], to_right)
    state = local_call(
        first_body, place, [*own, *inner, *queries], [TURNED, MIXED, PEAK], flops_of(8)
    )
    turned_q, mixed, peak = state
    right_outer = send(outer[0], to_left)
    left_outer = send(outer[1], to_right)
    mixed, peak = local_call(
        second_body, place, [*outer, turned_q, mixed, peak], [MIXED, PEAK],
        flops_of(4), aliases={4: 0, 5: 1},
    )
    right_inner, left_inner = send(right, partner), send(left, partner)
    mixed, peak = local_call(
        third_body, place, [left, left_inner, right, right_inner, turned_q, mixed, peak],
        [MIXED, PEAK], flops_of(4), aliases={6: 0, 7: 1},
    )
    outs = last(place, [left_outer, right_outer, turned_q, mixed, peak], flops_of(1))
    chunks = [send(outs[s], back_to_tiles(s)) for s in range(4)]
    away = terms(place, chunks, out_weight, False)
    arrived = send(away, partner)
    here = terms(place, chunks, out_weight, True)
    branch = local_call(
        close_body, place, [here, arrived, gate.reshape(1, -1)],
        jax.ShapeDtypeStruct((TILE, features), BF16),
    )
    return branch.reshape(1, 1, 1, TILE, features)


def solution(mesh):
    spec = P("ta", "ha", "wa", None, "grp")

    return jax.shard_map(
        shards,
        mesh=mesh,
        in_specs=(spec, spec, spec, P("grp", None), P("grp")),
        out_specs=spec,
        check_vma=False,
    )
```

```python
import math

import jax
import jax.numpy as jnp
from jax import lax
from jax.experimental import pallas as pl
from jax.experimental.pallas import tpu as pltpu
from jax.sharding import PartitionSpec as P


HD = 128
TILE = 256
AXES = ("grp", "ta", "ha", "wa")
FLIP = (0, 1, 1, 0)
HEADS = 3
ROWS = 144
LIMIT = 2.0**100
SCALE = HD**-0.5 * math.log2(math.e)
F32 = jnp.float32
BF16 = jnp.bfloat16


def flat(core, y, z, x):
    return ((core * 4 + y) * 2 + z % 2) * 8 + x * 2 + z // 2


def pairs(move):
    found = []
    for core in range(2):
        for y in range(4):
            for z in range(4):
                for x in range(4):
                    there = move(core, y, z, x)
                    if there is not None:
                        found.append((flat(core, y, z, x), flat(*there)))
    return sorted(found)


def out_to_heads(step):
    def move(core, y, z, x):
        half = y // 2
        return FLIP[y], (core if half == 0 else 3 - core), (z + step) % 4, x

    return pairs(move)


def back_to_tiles(step):
    return sorted((b, a) for a, b in out_to_heads(step))


def to_partner(core, y, z, x):
    return 1 - core, y, z, x


def to_outer(core, y, z, x):
    return (core, 3 - y, z, x) if core == 1 else None


def send(x, perm):
    return lax.ppermute(x, AXES, perm)


def turned(block):
    across = block.T
    return across[:, :HD], across[:, HD:]


def slot_cols(place, step, head):
    at = ((place[0] + step) % 4) * HEADS + head
    return pl.ds(pl.multiple_of(at * HD, HD), HD)


def pack_body(place, k_in, v_in, *outs):
    for step in range(4):
        for head in range(HEADS):
            cols = slot_cols(place, step, head)
            outs[step][head, 0] = k_in[:, cols]
            outs[step][head, 1, :HD], outs[step][head, 1, HD:] = turned(v_in[:, cols])


def pack_q_body(place, q_in, *outs):
    for step in range(4):
        for head in range(HEADS):
            outs[step][head, :HD], outs[step][head, HD:] = turned(
                q_in[:, slot_cols(place, step, head)]
            )


VMEM = pl.BlockSpec(memory_space=pltpu.MemorySpace.VMEM)
SMEM = pl.BlockSpec(memory_space=pltpu.MemorySpace.SMEM)


def local_call(body, place, operands, shapes, flops=0, limit=24, aliases=None):
    single = not isinstance(shapes, (list, tuple))
    listed = [shapes] if single else list(shapes)
    moved = sum(math.prod(a.shape) * a.dtype.itemsize for a in list(operands) + listed)
    return pl.pallas_call(
        body,
        in_specs=[SMEM] + [VMEM] * len(operands),
        out_specs=VMEM if single else [VMEM] * len(listed),
        out_shape=shapes,
        cost_estimate=pl.CostEstimate(flops=flops, bytes_accessed=moved, transcendentals=0),
        compiler_params=pltpu.CompilerParams(vmem_limit_bytes=limit * 1024 * 1024),
        input_output_aliases=aliases or {},
    )(place, *operands)


def gather_body(place, *refs):
    chunks, halves, whole = refs[:4], refs[4:6], refs[6]
    for step in range(4):
        z_from = (place[0] - step + 4) % 4
        whole[z_from // 2, :, z_from % 2] = chunks[step][...]
        for high in range(2):

            @pl.when(z_from // 2 == high)
            def _():
                halves[high][:, z_from % 2] = chunks[step][...]


MIXED = jax.ShapeDtypeStruct((HEADS, 2, ROWS, 2 * TILE), F32)
PEAK = jax.ShapeDtypeStruct((HEADS, 2, 1, 2 * TILE), F32)
TURNED = jax.ShapeDtypeStruct((HEADS, 4, 2 * HD, TILE), BF16)


def spread(place, q_in, turned_q):
    for step in range(4):
        z_from = (place[0] - step + 4) % 4
        for head in range(HEADS):
            both = jnp.concatenate([q_in[step][head, :HD], q_in[step][head, HD:]], axis=1)
            scaled = both.astype(F32) * SCALE
            high = scaled.astype(BF16)
            turned_q[head, z_from, :HD] = high
            turned_q[head, z_from, HD:] = (scaled - high.astype(F32)).astype(BF16)


def loaded(tiles):
    keys = jnp.concatenate([ref[head, low, 0] for ref, head, low in tiles], axis=0)
    values = jnp.concatenate(
        [
            ref[head, low, 1, half * HD : (half + 1) * HD]
            for ref, head, low in tiles
            for half in range(2)
        ],
        axis=1,
    )
    return keys, jnp.concatenate([values, jnp.ones((ROWS - HD, values.shape[1]), BF16)], axis=0)


def queries_of(turned_q, head, side):
    return jnp.concatenate([turned_q[head, 2 * side], turned_q[head, 2 * side + 1]], axis=1)


def scored(keys, queries):
    return jnp.dot(jnp.concatenate([keys, keys], axis=1), queries, preferred_element_type=F32)


def quick(queries, tiles, level, bias=None):
    keys, values = loaded(tiles)
    scores = scored(keys, queries) - (level if bias is None else level - bias)
    return jnp.dot(values, jnp.exp2(scores).astype(BF16), preferred_element_type=F32)


def careful(turned_q, mixed, peak, head, side, ref, bias=0.0):
    def one(low, carry):
        keys, values = loaded([(ref, head, low)])
        scores = scored(keys, queries_of(turned_q, head, side)) + bias
        before = peak[head, side]
        top = jnp.maximum(before, jnp.max(scores, axis=0, keepdims=True))
        probs = jnp.exp2(scores - top).astype(BF16)
        fresh = jnp.dot(values, probs, preferred_element_type=F32)
        mixed[head, side] = mixed[head, side] * jnp.exp2(before - top) + fresh
        peak[head, side] = top
        return carry

    lax.fori_loop(0, 2, one, 0)


def both_lows(head, *refs):
    return [(ref, head, low) for ref in refs for low in range(2)]


def within(sums):
    return jnp.max(sums) < LIMIT


def redo(turned_q, mixed, peak, shares, biases=(0.0, 0.0)):
    def one(head, carry):
        for side in range(2):
            for ref in shares[side]:
                careful(turned_q, mixed, peak, head, side, ref, biases[side])
        return carry

    lax.fori_loop(0, HEADS, one, 0)


def redo_alike(turned_q, mixed, peak, refs):
    def one(at, carry):
        for ref in refs:
            careful(turned_q, mixed, peak, at // 2, at % 2, ref)
        return carry

    lax.fori_loop(0, 2 * HEADS, one, 0)


def copied(source, target):
    def one(head, carry):
        target[head] = source[head]
        return carry

    lax.fori_loop(0, HEADS, one, 0)


def larger(one, two):
    return two if one is None else jnp.maximum(one, two)


def first_body(place, *refs):
    own, inner, q_in, (turned_q, mixed, peak) = refs[:2], refs[2], refs[3:7], refs[7:]
    inner = (inner.at[0], inner.at[1])
    spread(place, q_in, turned_q)

    def one(head, worst):
        for side in range(2):
            queries = queries_of(turned_q, head, side)
            level = jnp.max(scored(own[0][head, 0, 0, :HD], queries), axis=0, keepdims=True)
            peak[head, side] = level
            fresh = quick(queries, both_lows(head, *own), level) + quick(
                queries, both_lows(head, *inner), level
            )
            mixed[head, side] = fresh
            worst = jnp.maximum(worst, fresh[HD : HD + 8])
        return worst

    worst = lax.fori_loop(0, HEADS, one, jnp.zeros((8, 2 * TILE), F32))

    @pl.when(jnp.logical_not(within(worst)))
    def _():
        mixed[...] = jnp.zeros_like(mixed)
        redo_alike(turned_q, mixed, peak, (*own, *inner))


def more(turned_q, mixed_in, mixed, peak, shares, biases=(None, None)):
    worst = None
    for head in range(HEADS):
        for side in range(2):
            queries = queries_of(turned_q, head, side)
            fresh = mixed_in[head, side] + quick(
                queries, both_lows(head, *shares[side]), peak[head, side], biases[side]
            )
            mixed[head, side] = fresh
            worst = larger(worst, fresh[HD : HD + 8])
    return within(worst)


def edge_biases(place):
    return [jnp.where(place[2] == end, -1e30, 0.0).astype(F32) for end in (0, 3)]


def second_body(place, *refs):
    outer, (turned_q, mixed_in, _, mixed, peak) = refs[:2], refs[2:]

    @pl.when(place[1] == 0)
    def _():
        copied(mixed_in, mixed)

    @pl.when(place[1] == 1)
    def _():
        good = more(turned_q, mixed_in, mixed, peak, (outer, outer))

        @pl.when(jnp.logical_not(good))
        def _():
            copied(mixed_in, mixed)
            redo_alike(turned_q, mixed, peak, outer)


def third_body(place, *refs):
    left, right, turned_q, mixed_in, _, mixed, peak = refs
    biases = edge_biases(place)
    good = more(turned_q, mixed_in, mixed, peak, ((left,), (right,)), biases)

    @pl.when(jnp.logical_not(good))
    def _():
        copied(mixed_in, mixed)
        redo(turned_q, mixed, peak, ((left,), (right,)), biases)


def last_body(place, *refs):
    left, right, turned_q, mixed_in = refs[:2], refs[2:4], refs[4], refs[5]
    outs, (peak, mixed, done) = refs[7:11], refs[11:]
    biases = edge_biases(place)

    def passes(shares):
        good = more(turned_q, mixed_in, mixed, peak, shares, biases)

        @pl.when(jnp.logical_not(good))
        def _():
            copied(mixed_in, mixed)
            redo(turned_q, mixed, peak, shares, biases)

    @pl.when(place[1] == 1)
    def _():
        passes((left, right))

    @pl.when(place[1] == 0)
    def _():
        passes((left[:1], right[:1]))

    for head in range(HEADS):
        for side in range(2):
            inverse = 1.0 / mixed[head, side, HD : HD + 1]
            result = (mixed[head, side, :HD] * inverse).astype(BF16).T
            for low in range(2):
                done[2 * side + low, head] = result[low * TILE : (low + 1) * TILE]

    for step in range(4):
        z_from = (place[0] - step + 4) % 4
        for head in range(HEADS):
            outs[step][:, head * HD : (head + 1) * HD] = done[z_from, head]


def last(place, operands, flops):
    out = jax.ShapeDtypeStruct((TILE, HEADS * HD), BF16)
    return pl.pallas_call(
        last_body,
        in_specs=[SMEM] + [VMEM] * len(operands),
        out_specs=[VMEM] * 5,
        out_shape=[out] * 4 + [PEAK],
        scratch_shapes=[pltpu.VMEM(MIXED.shape, F32), pltpu.VMEM((4, HEADS, TILE, HD), BF16)],
        input_output_aliases={7: 4},
        cost_estimate=pl.CostEstimate(flops=flops, bytes_accessed=1 << 20, transcendentals=0),
        compiler_params=pltpu.CompilerParams(vmem_limit_bytes=24 * 1024 * 1024),
        name="last",
    )(place, *operands)[:4]


def join_body(place, *refs):
    chunks, joined = refs[:4], refs[4]
    for step in range(4):
        for head in range(HEADS):
            joined[:, slot_cols(place, step, head)] = chunks[step][:, head * HD : (head + 1) * HD]


def own_cols(core, width):
    return pl.ds(pl.multiple_of(core * width, width), width)


def home_body(place, joined, weight, out):
    cols = own_cols(place[1], out.shape[1])
    out[...] = jnp.dot(joined[...], weight[:, cols], preferred_element_type=F32)


def cut_body(place, weight, out):
    out[...] = weight[:, own_cols(1 - place[1], out.shape[1])]


def close_body(place, here, joined, weight, gate, out):
    there = jnp.dot(joined[...], weight[...], preferred_element_type=F32)
    out[...] = (gate[...].astype(F32) * (here[...] + there)).astype(BF16)


def shards(query_tiles, key_tiles, value_tiles, out_weight, gate):
    features = query_tiles.shape[4]
    q, k, v = (a.reshape(TILE, features) for a in (query_tiles, key_tiles, value_tiles))
    core, y = lax.axis_index("grp"), lax.axis_index("ta")
    wide = lax.axis_index("wa")
    z, x = (wide % 2) * 2 + lax.axis_index("ha"), wide // 2
    place = jnp.stack([z, core, x, y]).astype(jnp.int32)
    partner, outer_pairs = pairs(to_partner), pairs(to_outer)
    to_right = pairs(lambda core, y, z, x: (core, y, z, x + 1) if x < 3 else None)
    to_left = pairs(lambda core, y, z, x: (core, y, z, x - 1) if x > 0 else None)
    upper = flat(1, 0, 0, 0)
    right_upper, left_upper = ([p for p in perm if p[0] >= upper] for perm in (to_right, to_left))
    flops_of = lambda tiles: HEADS * 4 * TILE * tiles * TILE * 6 * HD

    kv_shape = jax.ShapeDtypeStruct((HEADS, 2, TILE, HD), BF16)
    kv_sent = local_call(pack_body, place, [k, v], [kv_shape] * 4)
    kv = [send(kv_sent[s], out_to_heads(s)) for s in range(4)]
    q_shape = jax.ShapeDtypeStruct((HEADS, TILE, HD), BF16)
    q_sent = local_call(pack_q_body, place, [q], [q_shape] * 4)
    queries = [send(q_sent[s], out_to_heads(s)) for s in range(4)]
    weight_away = local_call(
        cut_body, place, [out_weight], jax.ShapeDtypeStruct((features, features), BF16)
    )
    weight_other = send(weight_away, partner)
    half = (HEADS, 2, 2, TILE, HD)
    *own, whole = local_call(
        gather_body, place, kv,
        [jax.ShapeDtypeStruct(half, BF16)] * 2 + [jax.ShapeDtypeStruct((2, *half), BF16)],
    )
    outer = [send(own[i], outer_pairs) for i in range(2)]
    inner = send(whole, partner)
    right, left = send(own[0], to_left), send(own[1], to_right)
    state = local_call(
        first_body, place, [*own, inner, *queries], [TURNED, MIXED, PEAK], flops_of(8)
    )
    turned_q, mixed, peak = state
    right_outer = send(outer[0], left_upper)
    left_outer = send(outer[1], right_upper)
    mixed, peak = local_call(
        second_body, place, [*outer, turned_q, mixed, peak], [MIXED, PEAK],
        flops_of(4), aliases={5: 1},
    )
    right_inner, left_inner = send(right, partner), send(left, partner)
    mixed, peak = local_call(
        third_body, place, [left, right, turned_q, mixed, peak],
        [MIXED, PEAK], flops_of(2), aliases={5: 1},
    )
    outs = last(
        place, [left_inner, left_outer, right_inner, right_outer, turned_q, mixed, peak], flops_of(4)
    )
    chunks = [send(outs[s], back_to_tiles(s)) for s in range(4)]
    joined = local_call(join_body, place, chunks, jax.ShapeDtypeStruct((TILE, features), BF16))
    arrived = send(joined, partner)
    flops = 2 * TILE * features * features
    here = local_call(
        home_body, place, [joined, out_weight], jax.ShapeDtypeStruct((TILE, features), F32), flops
    )
    branch = local_call(
        close_body, place, [here, arrived, weight_other, gate.reshape(1, -1)],
        jax.ShapeDtypeStruct((TILE, features), BF16), flops,
    )
    return branch.reshape(1, 1, 1, TILE, features)


def solution(mesh):
    spec = P("ta", "ha", "wa", None, "grp")

    return jax.shard_map(
        shards,
        mesh=mesh,
        in_specs=(spec, spec, spec, P("grp", None), P("grp")),
        out_specs=spec,
        check_vma=False,
    )
```

```python
import functools
import math

import jax
import jax.numpy as jnp
from jax import lax
from jax.experimental import pallas as pl
from jax.experimental.pallas import tpu as pltpu
from jax.sharding import PartitionSpec as P


HD = 128
TILE = 256
AXES = ("grp", "ta", "ha", "wa")
FLIP = (0, 1, 1, 0)
HEADS = 3
ROWS = 144
LIMIT = 2.0**100
SCALE = HD**-0.5 * math.log2(math.e)
F32 = jnp.float32
BF16 = jnp.bfloat16


def flat(core, y, z, x):
    return ((core * 4 + y) * 2 + z % 2) * 8 + x * 2 + z // 2


def pairs(move):
    found = []
    for core in range(2):
        for y in range(4):
            for z in range(4):
                for x in range(4):
                    there = move(core, y, z, x)
                    if there is not None:
                        found.append((flat(core, y, z, x), flat(*there)))
    return sorted(found)


def out_to_heads(step):
    def move(core, y, z, x):
        half = y // 2
        return FLIP[y], (core if half == 0 else 3 - core), (z + step) % 4, x

    return pairs(move)


def back_to_tiles(step):
    return sorted((b, a) for a, b in out_to_heads(step))


def to_partner(core, y, z, x):
    return 1 - core, y, z, x


def to_outer(core, y, z, x):
    return (core, 3 - y, z, x) if core == 1 else None


def to_near(core, y, z, x):
    return core, y, z, x ^ 1


def to_far(core, y, z, x):
    return (core, y, z, 3 - x) if x in (1, 2) else None


def send(x, perm):
    return lax.ppermute(x, AXES, perm)


def turned(block):
    across = block.T
    return across[:, :HD], across[:, HD:]


def slot_cols(place, step, head):
    at = ((place[0] + step) % 4) * HEADS + head
    return pl.ds(pl.multiple_of(at * HD, HD), HD)


def pack_body(place, k_in, v_in, *outs):
    for step in range(4):
        for head in range(HEADS):
            cols = slot_cols(place, step, head)
            outs[step][head, 0] = k_in[:, cols]
            outs[step][head, 1, :HD], outs[step][head, 1, HD:] = turned(v_in[:, cols])


def pack_q_body(place, q_in, *outs):
    for step in range(4):
        for head in range(HEADS):
            outs[step][head, :HD], outs[step][head, HD:] = turned(
                q_in[:, slot_cols(place, step, head)]
            )


def placed():
    wide = lax.axis_index("wa")
    return (wide & 1) * 2 + lax.axis_index("ha"), lax.axis_index("grp"), wide >> 1, lax.axis_index("ta")


def here_body(body, *refs):
    body(placed(), *refs)


VMEM = pl.BlockSpec(memory_space=pltpu.MemorySpace.VMEM)


def local_call(body, operands, shapes, flops=0, limit=24, aliases=None):
    single = not isinstance(shapes, (list, tuple))
    listed = [shapes] if single else list(shapes)
    moved = sum(math.prod(a.shape) * a.dtype.itemsize for a in list(operands) + listed)
    return pl.pallas_call(
        functools.partial(here_body, body),
        in_specs=[VMEM] * len(operands),
        out_specs=VMEM if single else [VMEM] * len(listed),
        out_shape=shapes,
        cost_estimate=pl.CostEstimate(flops=flops, bytes_accessed=moved, transcendentals=0),
        compiler_params=pltpu.CompilerParams(vmem_limit_bytes=limit * 1024 * 1024),
        input_output_aliases=aliases or {},
    )(*operands)


def gather_body(place, *refs):
    chunks, halves, whole = refs[:4], refs[4:6], refs[6]
    for step in range(4):
        z_from = (place[0] - step + 4) % 4
        whole[z_from // 2, :, z_from % 2] = chunks[step][...]
        beside_far = z_from // 2 == place[2] % 2
        for which, chosen in ((0, jnp.logical_not(beside_far)), (1, beside_far)):

            @pl.when(chosen)
            def _():
                halves[which][:, z_from % 2] = chunks[step][...]


MIXED = jax.ShapeDtypeStruct((HEADS, 2, ROWS, 2 * TILE), F32)
PEAK = jax.ShapeDtypeStruct((HEADS, 2, 1, 2 * TILE), F32)
TURNED = jax.ShapeDtypeStruct((HEADS, 4, 2 * HD, TILE), BF16)


def spread(place, q_in, turned_q):
    for step in range(4):
        z_from = (place[0] - step + 4) % 4
        for head in range(HEADS):
            both = jnp.concatenate([q_in[step][head, :HD], q_in[step][head, HD:]], axis=1)
            scaled = both.astype(F32) * SCALE
            high = scaled.astype(BF16)
            turned_q[head, z_from, :HD] = high
            turned_q[head, z_from, HD:] = (scaled - high.astype(F32)).astype(BF16)


def loaded(tiles):
    keys = jnp.concatenate([ref[head, low, 0] for ref, head, low in tiles], axis=0)
    values = jnp.concatenate(
        [
            ref[head, low, 1, half * HD : (half + 1) * HD]
            for ref, head, low in tiles
            for half in range(2)
        ],
        axis=1,
    )
    return keys, jnp.concatenate([values, jnp.ones((ROWS - HD, values.shape[1]), BF16)], axis=0)


def queries_of(turned_q, head, side):
    return jnp.concatenate([turned_q[head, 2 * side], turned_q[head, 2 * side + 1]], axis=1)


def scored(keys, queries):
    return jnp.dot(jnp.concatenate([keys, keys], axis=1), queries, preferred_element_type=F32)


def quick(queries, tiles, level, bias=None):
    keys, values = loaded(tiles)
    scores = scored(keys, queries) - (level if bias is None else level - bias)
    return jnp.dot(values, jnp.exp2(scores).astype(BF16), preferred_element_type=F32)


def careful(turned_q, mixed, peak, head, side, ref, bias=0.0):
    def one(low, carry):
        keys, values = loaded([(ref, head, low)])
        scores = scored(keys, queries_of(turned_q, head, side)) + bias
        before = peak[head, side]
        top = jnp.maximum(before, jnp.max(scores, axis=0, keepdims=True))
        probs = jnp.exp2(scores - top).astype(BF16)
        fresh = jnp.dot(values, probs, preferred_element_type=F32)
        mixed[head, side] = mixed[head, side] * jnp.exp2(before - top) + fresh
        peak[head, side] = top
        return carry

    lax.fori_loop(0, 2, one, 0)


def both_lows(head, *refs):
    return [(ref, head, low) for ref in refs for low in range(2)]


def within(sums):
    return jnp.max(sums) < LIMIT


def redo(turned_q, mixed, peak, shares, sides, biases):
    def one(head, carry):
        for part in range(2):
            for ref in shares[part]:
                careful(turned_q, mixed, peak, head, sides[part], ref, 0.0 if part == 0 else biases[1])
        return carry

    lax.fori_loop(0, HEADS, one, 0)


def redo_alike(turned_q, mixed, peak, refs):
    def one(at, carry):
        for ref in refs:
            careful(turned_q, mixed, peak, at // 2, at % 2, ref)
        return carry

    lax.fori_loop(0, 2 * HEADS, one, 0)


def copied(source, target):
    def one(head, carry):
        target[head] = source[head]
        return carry

    lax.fori_loop(0, HEADS, one, 0)


def larger(one, two):
    return two if one is None else jnp.maximum(one, two)


def first_body(place, *refs):
    own, inner, q_in, (turned_q, mixed, peak) = refs[:2], refs[2], refs[3:7], refs[7:]
    inner = (inner.at[0], inner.at[1])
    spread(place, q_in, turned_q)

    def one(head, worst):
        for side in range(2):
            queries = queries_of(turned_q, head, side)
            level = jnp.max(scored(own[0][head, 0, 0, :HD], queries), axis=0, keepdims=True)
            peak[head, side] = level
            fresh = quick(queries, both_lows(head, *own), level) + quick(
                queries, both_lows(head, *inner), level
            )
            mixed[head, side] = fresh
            worst = jnp.maximum(worst, fresh[HD : HD + 8])
        return worst

    worst = jnp.zeros((8, 2 * TILE), F32)
    for head in range(HEADS):
        worst = one(head, worst)

    @pl.when(jnp.logical_not(within(worst)))
    def _():
        mixed[...] = jnp.zeros_like(mixed)
        redo_alike(turned_q, mixed, peak, (*own, *inner))


def more(turned_q, mixed_in, mixed, peak, shares, sides=(0, 1), biases=(None, None)):
    worst = None
    for head in range(HEADS):
        for part in range(2):
            side = sides[part]
            fresh = mixed_in[head, side] + quick(
                queries_of(turned_q, head, side),
                both_lows(head, *shares[part]),
                peak[head, side],
                biases[part],
            )
            mixed[head, side] = fresh
            worst = larger(worst, fresh[HD : HD + 8])
    return within(worst)


def edge_sides(place):
    far_side = place[2] % 2
    missing = jnp.logical_or(place[2] == 0, place[2] == 3)
    return (1 - far_side, far_side), (None, jnp.where(missing, -1e30, 0.0).astype(F32))


def second_body(place, *refs):
    outer, (turned_q, mixed_in, _, mixed, peak) = refs[:2], refs[2:]

    @pl.when(place[1] == 0)
    def _():
        copied(mixed_in, mixed)

    @pl.when(place[1] == 1)
    def _():
        good = more(turned_q, mixed_in, mixed, peak, (outer, outer))

        @pl.when(jnp.logical_not(good))
        def _():
            copied(mixed_in, mixed)
            redo_alike(turned_q, mixed, peak, outer)


def third_body(place, *refs):
    near, far, turned_q, mixed_in, _, mixed, peak = refs
    sides, biases = edge_sides(place)
    shares = (near,), (far,)
    good = more(turned_q, mixed_in, mixed, peak, shares, sides, biases)

    @pl.when(jnp.logical_not(good))
    def _():
        copied(mixed_in, mixed)
        redo(turned_q, mixed, peak, shares, sides, biases)


def last_body(place, *refs):
    near, far, turned_q, mixed_in = refs[:2], refs[2:4], refs[4], refs[5]
    outs, (peak, mixed, done) = refs[7:11], refs[11:]
    sides, biases = edge_sides(place)

    def passes(shares):
        good = more(turned_q, mixed_in, mixed, peak, shares, sides, biases)

        @pl.when(jnp.logical_not(good))
        def _():
            copied(mixed_in, mixed)
            redo(turned_q, mixed, peak, shares, sides, biases)

    @pl.when(place[1] == 1)
    def _():
        passes((near, far))

    @pl.when(place[1] == 0)
    def _():
        passes((near[:1], far[:1]))

    for head in range(HEADS):
        for side in range(2):
            inverse = 1.0 / mixed[head, side, HD : HD + 1]
            result = (mixed[head, side, :HD] * inverse).astype(BF16).T
            for low in range(2):
                done[2 * side + low, head] = result[low * TILE : (low + 1) * TILE]

    for step in range(4):
        z_from = (place[0] - step + 4) % 4
        for head in range(HEADS):
            outs[step][:, head * HD : (head + 1) * HD] = done[z_from, head]


def last(operands, flops):
    out = jax.ShapeDtypeStruct((TILE, HEADS * HD), BF16)
    return pl.pallas_call(
        functools.partial(here_body, last_body),
        in_specs=[VMEM] * len(operands),
        out_specs=[VMEM] * 5,
        out_shape=[out] * 4 + [PEAK],
        scratch_shapes=[pltpu.VMEM(MIXED.shape, F32), pltpu.VMEM((4, HEADS, TILE, HD), BF16)],
        input_output_aliases={6: 4},
        cost_estimate=pl.CostEstimate(flops=flops, bytes_accessed=1 << 20, transcendentals=0),
        compiler_params=pltpu.CompilerParams(vmem_limit_bytes=24 * 1024 * 1024),
        name="last",
    )(*operands)[:4]


def join_body(place, *refs):
    chunks, joined = refs[:4], refs[4]
    for step in range(4):
        for head in range(HEADS):
            joined[:, slot_cols(place, step, head)] = chunks[step][:, head * HD : (head + 1) * HD]


def own_cols(core, width):
    return pl.ds(pl.multiple_of(core * width, width), width)


def home_body(place, joined, weight, out):
    cols = own_cols(place[1], out.shape[1])
    out[...] = jnp.dot(joined[...], weight[:, cols], preferred_element_type=F32)


def cut_body(place, weight, out):
    out[...] = weight[:, own_cols(1 - place[1], out.shape[1])]


def close_body(place, here, joined, weight, gate, out):
    there = jnp.dot(joined[...], weight[...], preferred_element_type=F32)
    out[...] = (gate[...].astype(F32) * (here[...] + there)).astype(BF16)


def shards(query_tiles, key_tiles, value_tiles, out_weight, gate):
    features = query_tiles.shape[4]
    q, k, v = (a.reshape(TILE, features) for a in (query_tiles, key_tiles, value_tiles))
    partner, outer_pairs = pairs(to_partner), pairs(to_outer)
    near_pairs, far_pairs = pairs(to_near), pairs(to_far)
    upper = flat(1, 0, 0, 0)
    near_upper, far_upper = ([p for p in perm if p[0] >= upper] for perm in (near_pairs, far_pairs))
    flops_of = lambda tiles: HEADS * 4 * TILE * tiles * TILE * 6 * HD

    kv_shape = jax.ShapeDtypeStruct((HEADS, 2, TILE, HD), BF16)
    kv_sent = local_call(pack_body, [k, v], [kv_shape] * 4)
    kv = [send(kv_sent[s], out_to_heads(s)) for s in range(4)]
    q_shape = jax.ShapeDtypeStruct((HEADS, TILE, HD), BF16)
    q_sent = local_call(pack_q_body, [q], [q_shape] * 4)
    queries = [send(q_sent[s], out_to_heads(s)) for s in range(4)]
    weight_away = local_call(
        cut_body, [out_weight], jax.ShapeDtypeStruct((features, features), BF16)
    )
    weight_other = send(weight_away, partner)
    half = (HEADS, 2, 2, TILE, HD)
    *own, whole = local_call(
        gather_body, kv,
        [jax.ShapeDtypeStruct(half, BF16)] * 2 + [jax.ShapeDtypeStruct((2, *half), BF16)],
    )
    outer = [send(own[i], outer_pairs) for i in range(2)]
    inner = send(whole, partner)
    near, far = send(own[0], near_pairs), send(own[1], far_pairs)
    state = local_call(first_body, [*own, inner, *queries], [TURNED, MIXED, PEAK], flops_of(8))
    turned_q, mixed, peak = state
    near_outer = send(outer[0], near_upper)
    far_outer = send(outer[1], far_upper)
    mixed, peak = local_call(
        second_body, [*outer, turned_q, mixed, peak], [MIXED, PEAK],
        flops_of(4), aliases={4: 1},
    )
    near_inner, far_inner = send(near, partner), send(far, partner)
    mixed, peak = local_call(
        third_body, [near, far, turned_q, mixed, peak],
        [MIXED, PEAK], flops_of(2), aliases={4: 1},
    )
    outs = last(
        [near_inner, near_outer, far_inner, far_outer, turned_q, mixed, peak], flops_of(4)
    )
    chunks = [send(outs[s], back_to_tiles(s)) for s in range(4)]
    joined = local_call(join_body, chunks, jax.ShapeDtypeStruct((TILE, features), BF16))
    arrived = send(joined, partner)
    flops = 2 * TILE * features * features
    here = local_call(
        home_body, [joined, out_weight], jax.ShapeDtypeStruct((TILE, features), F32), flops
    )
    branch = local_call(
        close_body, [here, arrived, weight_other, gate.reshape(1, -1)],
        jax.ShapeDtypeStruct((TILE, features), BF16), flops,
    )
    return branch.reshape(1, 1, 1, TILE, features)


def solution(mesh):
    spec = P("ta", "ha", "wa", None, "grp")

    return jax.shard_map(
        shards,
        mesh=mesh,
        in_specs=(spec, spec, spec, P("grp", None), P("grp")),
        out_specs=spec,
        check_vma=False,
    )
```

```python
import functools
import math

import jax
import jax.numpy as jnp
from jax import lax
from jax.experimental import pallas as pl
from jax.experimental.pallas import tpu as pltpu
from jax.sharding import PartitionSpec as P


HD = 128
TILE = 256
AXES = ("grp", "ta", "ha", "wa")
FLIP = (0, 1, 1, 0)
HEADS = 3
ROWS = 144
LIMIT = 2.0**100
SCALE = HD**-0.5 * math.log2(math.e)
F32 = jnp.float32
BF16 = jnp.bfloat16


def flat(core, y, z, x):
    return ((core * 4 + y) * 2 + z % 2) * 8 + x * 2 + z // 2


def pairs(move):
    found = []
    for core in range(2):
        for y in range(4):
            for z in range(4):
                for x in range(4):
                    there = move(core, y, z, x)
                    if there is not None:
                        found.append((flat(core, y, z, x), flat(*there)))
    return sorted(found)


def out_to_heads(step):
    def move(core, y, z, x):
        half = y // 2
        return FLIP[y], (core if half == 0 else 3 - core), (z + step) % 4, x

    return pairs(move)


def back_to_tiles(step):
    return sorted((b, a) for a, b in out_to_heads(step))


def to_partner(core, y, z, x):
    return 1 - core, y, z, x


def to_outer(core, y, z, x):
    return (core, 3 - y, z, x) if core == 1 else None


def to_near(core, y, z, x):
    return core, y, z, x ^ 1


def to_far(core, y, z, x):
    return (core, y, z, 3 - x) if x in (1, 2) else None


def send(x, perm):
    return lax.ppermute(x, AXES, perm)


def turned(block):
    across = block.T
    return across[:, :HD], across[:, HD:]


def slot_cols(place, step, head):
    at = ((place[0] + step) % 4) * HEADS + head
    return pl.ds(pl.multiple_of(at * HD, HD), HD)


def pack_body(place, k_in, v_in, *outs):
    for step in range(4):
        for head in range(HEADS):
            cols = slot_cols(place, step, head)
            outs[step][head, 0] = k_in[:, cols]
            outs[step][head, 1, :HD], outs[step][head, 1, HD:] = turned(v_in[:, cols])


def pack_q_body(place, q_in, *outs):
    for step in range(4):
        for head in range(HEADS):
            outs[step][head, :HD], outs[step][head, HD:] = turned(
                q_in[:, slot_cols(place, step, head)]
            )


def placed():
    wide = lax.axis_index("wa")
    return (wide & 1) * 2 + lax.axis_index("ha"), lax.axis_index("grp"), wide >> 1, lax.axis_index("ta")


def here_body(body, *refs):
    body(placed(), *refs)


VMEM = pl.BlockSpec(memory_space=pltpu.MemorySpace.VMEM)


def local_call(body, operands, shapes, flops=0, limit=24, aliases=None):
    single = not isinstance(shapes, (list, tuple))
    listed = [shapes] if single else list(shapes)
    moved = sum(math.prod(a.shape) * a.dtype.itemsize for a in list(operands) + listed)
    return pl.pallas_call(
        functools.partial(here_body, body),
        in_specs=[VMEM] * len(operands),
        out_specs=VMEM if single else [VMEM] * len(listed),
        out_shape=shapes,
        cost_estimate=pl.CostEstimate(flops=flops, bytes_accessed=moved, transcendentals=0),
        compiler_params=pltpu.CompilerParams(vmem_limit_bytes=limit * 1024 * 1024),
        input_output_aliases=aliases or {},
    )(*operands)


def gather_body(place, *refs):
    chunks, halves, whole = refs[:4], refs[4:6], refs[6]
    for step in range(4):
        z_from = (place[0] - step + 4) % 4
        whole[z_from // 2, :, z_from % 2] = chunks[step][...]
        beside_far = z_from // 2 == place[2] % 2
        for which, chosen in ((0, jnp.logical_not(beside_far)), (1, beside_far)):

            @pl.when(chosen)
            def _():
                halves[which][:, z_from % 2] = chunks[step][...]


MIXED = jax.ShapeDtypeStruct((HEADS, 2, ROWS, 2 * TILE), F32)
PEAK = jax.ShapeDtypeStruct((HEADS, 2, 1, 2 * TILE), F32)
TURNED = jax.ShapeDtypeStruct((HEADS, 4, 2 * HD, TILE), BF16)


def spread(place, q_in, turned_q):
    for step in range(4):
        z_from = (place[0] - step + 4) % 4
        for head in range(HEADS):
            both = jnp.concatenate([q_in[step][head, :HD], q_in[step][head, HD:]], axis=1)
            scaled = both.astype(F32) * SCALE
            high = scaled.astype(BF16)
            turned_q[head, z_from, :HD] = high
            turned_q[head, z_from, HD:] = (scaled - high.astype(F32)).astype(BF16)


def loaded(tiles):
    keys = jnp.concatenate([ref[head, low, 0] for ref, head, low in tiles], axis=0)
    values = jnp.concatenate(
        [
            ref[head, low, 1, half * HD : (half + 1) * HD]
            for ref, head, low in tiles
            for half in range(2)
        ],
        axis=1,
    )
    return keys, jnp.concatenate([values, jnp.ones((ROWS - HD, values.shape[1]), BF16)], axis=0)


def queries_of(turned_q, head, side):
    return jnp.concatenate([turned_q[head, 2 * side], turned_q[head, 2 * side + 1]], axis=1)


def scored(keys, queries):
    return jnp.dot(jnp.concatenate([keys, keys], axis=1), queries, preferred_element_type=F32)


def quick(queries, tiles, level, bias=None):
    keys, values = loaded(tiles)
    scores = scored(keys, queries) - (level if bias is None else level - bias)
    return jnp.dot(values, jnp.exp2(scores).astype(BF16), preferred_element_type=F32)


def careful(turned_q, mixed, peak, head, side, ref, bias=0.0):
    def one(low, carry):
        keys, values = loaded([(ref, head, low)])
        scores = scored(keys, queries_of(turned_q, head, side)) + bias
        before = peak[head, side]
        top = jnp.maximum(before, jnp.max(scores, axis=0, keepdims=True))
        probs = jnp.exp2(scores - top).astype(BF16)
        fresh = jnp.dot(values, probs, preferred_element_type=F32)
        mixed[head, side] = mixed[head, side] * jnp.exp2(before - top) + fresh
        peak[head, side] = top
        return carry

    lax.fori_loop(0, 2, one, 0)


def both_lows(head, *refs):
    return [(ref, head, low) for ref in refs for low in range(2)]


def within(sums):
    return jnp.max(sums) < LIMIT


def redo(turned_q, mixed, peak, shares, sides, biases):
    def one(head, carry):
        for part in range(2):
            for ref in shares[part]:
                careful(turned_q, mixed, peak, head, sides[part], ref, 0.0 if part == 0 else biases[1])
        return carry

    lax.fori_loop(0, HEADS, one, 0)


def redo_alike(turned_q, mixed, peak, refs):
    def one(at, carry):
        for ref in refs:
            careful(turned_q, mixed, peak, at // 2, at % 2, ref)
        return carry

    lax.fori_loop(0, 2 * HEADS, one, 0)


def copied(source, target):
    def one(head, carry):
        target[head] = source[head]
        return carry

    lax.fori_loop(0, HEADS, one, 0)


def larger(one, two):
    return two if one is None else jnp.maximum(one, two)


def first_body(place, *refs):
    own, inner, q_in, (turned_q, mixed, peak) = refs[:2], refs[2], refs[3:7], refs[7:]
    inner = (inner.at[0], inner.at[1])
    spread(place, q_in, turned_q)

    def one(head, worst):
        for side in range(2):
            queries = queries_of(turned_q, head, side)
            level = jnp.max(scored(own[0][head, 0, 0, :HD], queries), axis=0, keepdims=True)
            peak[head, side] = level
            fresh = quick(queries, both_lows(head, *own), level) + quick(
                queries, both_lows(head, *inner), level
            )
            mixed[head, side] = fresh
            worst = jnp.maximum(worst, fresh[HD : HD + 8])
        return worst

    worst = jnp.zeros((8, 2 * TILE), F32)
    for head in range(HEADS):
        worst = one(head, worst)

    @pl.when(jnp.logical_not(within(worst)))
    def _():
        mixed[...] = jnp.zeros_like(mixed)
        redo_alike(turned_q, mixed, peak, (*own, *inner))


def more(turned_q, mixed_in, mixed, peak, shares, sides=(0, 1), biases=(None, None)):
    worst = None
    for head in range(HEADS):
        for part in range(2):
            side = sides[part]
            fresh = mixed_in[head, side] + quick(
                queries_of(turned_q, head, side),
                both_lows(head, *shares[part]),
                peak[head, side],
                biases[part],
            )
            mixed[head, side] = fresh
            worst = larger(worst, fresh[HD : HD + 8])
    return within(worst)


def edge_sides(place):
    far_side = place[2] % 2
    missing = jnp.logical_or(place[2] == 0, place[2] == 3)
    return (1 - far_side, far_side), (None, jnp.where(missing, -1e30, 0.0).astype(F32))


def second_body(place, *refs):
    outer, (turned_q, mixed_in, _, mixed, peak) = refs[:2], refs[2:]

    @pl.when(place[1] == 0)
    def _():
        copied(mixed_in, mixed)

    @pl.when(place[1] == 1)
    def _():
        good = more(turned_q, mixed_in, mixed, peak, (outer, outer))

        @pl.when(jnp.logical_not(good))
        def _():
            copied(mixed_in, mixed)
            redo_alike(turned_q, mixed, peak, outer)


def third_body(place, *refs):
    near, far, turned_q, mixed_in, _, mixed, peak = refs
    sides, biases = edge_sides(place)
    shares = (near,), (far,)
    good = more(turned_q, mixed_in, mixed, peak, shares, sides, biases)

    @pl.when(jnp.logical_not(good))
    def _():
        copied(mixed_in, mixed)
        redo(turned_q, mixed, peak, shares, sides, biases)


def last_body(place, *refs):
    outs, (peak, mixed, done) = refs[5:9], refs[9:]

    @pl.when(place[1] == 1)
    def _():
        third_body(place, *refs[:5], mixed, peak)

    @pl.when(place[1] == 0)
    def _():
        copied(refs[3], mixed)

    for head in range(HEADS):
        for side in range(2):
            inverse = 1.0 / mixed[head, side, HD : HD + 1]
            result = (mixed[head, side, :HD] * inverse).astype(BF16).T
            for low in range(2):
                done[2 * side + low, head] = result[low * TILE : (low + 1) * TILE]

    for step in range(4):
        z_from = (place[0] - step + 4) % 4
        for head in range(HEADS):
            outs[step][:, head * HD : (head + 1) * HD] = done[z_from, head]


def last(operands, flops):
    out = jax.ShapeDtypeStruct((TILE, HEADS * HD), BF16)
    return pl.pallas_call(
        functools.partial(here_body, last_body),
        in_specs=[VMEM] * len(operands),
        out_specs=[VMEM] * 5,
        out_shape=[out] * 4 + [PEAK],
        scratch_shapes=[pltpu.VMEM(MIXED.shape, F32), pltpu.VMEM((4, HEADS, TILE, HD), BF16)],
        input_output_aliases={4: 4},
        cost_estimate=pl.CostEstimate(flops=flops, bytes_accessed=1 << 20, transcendentals=0),
        compiler_params=pltpu.CompilerParams(vmem_limit_bytes=24 * 1024 * 1024),
        name="last",
    )(*operands)[:4]


def join_body(place, *refs):
    chunks, joined = refs[:4], refs[4]
    for step in range(4):
        for head in range(HEADS):
            joined[:, slot_cols(place, step, head)] = chunks[step][:, head * HD : (head + 1) * HD]


def own_cols(core, width):
    return pl.ds(pl.multiple_of(core * width, width), width)


def home_body(place, joined, weight, out):
    cols = own_cols(place[1], out.shape[1])
    out[...] = jnp.dot(joined[...], weight[:, cols], preferred_element_type=F32)


def cut_body(place, weight, out):
    out[...] = weight[:, own_cols(1 - place[1], out.shape[1])]


def close_body(place, here, joined, weight, gate, out):
    there = jnp.dot(joined[...], weight[...], preferred_element_type=F32)
    out[...] = (gate[...].astype(F32) * (here[...] + there)).astype(BF16)


def shards(query_tiles, key_tiles, value_tiles, out_weight, gate):
    features = query_tiles.shape[4]
    q, k, v = (a.reshape(TILE, features) for a in (query_tiles, key_tiles, value_tiles))
    partner, outer_pairs = pairs(to_partner), pairs(to_outer)
    near_pairs, far_pairs = pairs(to_near), pairs(to_far)
    upper = flat(1, 0, 0, 0)
    near_upper, far_upper = ([p for p in perm if p[0] >= upper] for perm in (near_pairs, far_pairs))
    flops_of = lambda tiles: HEADS * 4 * TILE * tiles * TILE * 6 * HD

    kv_shape = jax.ShapeDtypeStruct((HEADS, 2, TILE, HD), BF16)
    kv_sent = local_call(pack_body, [k, v], [kv_shape] * 4)
    kv = [send(kv_sent[s], out_to_heads(s)) for s in range(4)]
    q_shape = jax.ShapeDtypeStruct((HEADS, TILE, HD), BF16)
    q_sent = local_call(pack_q_body, [q], [q_shape] * 4)
    queries = [send(q_sent[s], out_to_heads(s)) for s in range(4)]
    weight_away = local_call(
        cut_body, [out_weight], jax.ShapeDtypeStruct((features, features), BF16)
    )
    weight_other = send(weight_away, partner)
    half = (HEADS, 2, 2, TILE, HD)
    *own, whole = local_call(
        gather_body, kv,
        [jax.ShapeDtypeStruct(half, BF16)] * 2 + [jax.ShapeDtypeStruct((2, *half), BF16)],
    )
    outer = [send(own[i], outer_pairs) for i in range(2)]
    inner = send(whole, partner)
    near, far = send(own[0], near_pairs), send(own[1], far_pairs)
    state = local_call(first_body, [*own, inner, *queries], [TURNED, MIXED, PEAK], flops_of(8))
    turned_q, mixed, peak = state
    near_outer = send(outer[0], near_upper)
    far_outer = send(outer[1], far_upper)
    mixed, peak = local_call(
        second_body, [*outer, turned_q, mixed, peak], [MIXED, PEAK],
        flops_of(4), aliases={4: 1},
    )
    near_inner, far_inner = send(near, partner), send(far, partner)
    mixed, peak = local_call(
        third_body, [near, far, turned_q, mixed, peak],
        [MIXED, PEAK], flops_of(2), aliases={4: 1},
    )
    mixed, peak = local_call(
        third_body, [near_inner, far_inner, turned_q, mixed, peak],
        [MIXED, PEAK], flops_of(2), aliases={4: 1},
    )
    outs = last([near_outer, far_outer, turned_q, mixed, peak], flops_of(2))
    chunks = [send(outs[s], back_to_tiles(s)) for s in range(4)]
    joined = local_call(join_body, chunks, jax.ShapeDtypeStruct((TILE, features), BF16))
    arrived = send(joined, partner)
    flops = 2 * TILE * features * features
    here = local_call(
        home_body, [joined, out_weight], jax.ShapeDtypeStruct((TILE, features), F32), flops
    )
    branch = local_call(
        close_body, [here, arrived, weight_other, gate.reshape(1, -1)],
        jax.ShapeDtypeStruct((TILE, features), BF16), flops,
    )
    return branch.reshape(1, 1, 1, TILE, features)


def solution(mesh):
    spec = P("ta", "ha", "wa", None, "grp")

    return jax.shard_map(
        shards,
        mesh=mesh,
        in_specs=(spec, spec, spec, P("grp", None), P("grp")),
        out_specs=spec,
        check_vma=False,
    )
```

```python
import functools
import math

import jax
import jax.numpy as jnp
from jax import lax
from jax.experimental import pallas as pl
from jax.experimental.pallas import tpu as pltpu
from jax.sharding import PartitionSpec as P


HD = 128
TILE = 256
AXES = ("grp", "ta", "ha", "wa")
FLIP = (0, 1, 1, 0)
HEADS = 3
ROWS = 144
LIMIT = 2.0**100
SCALE = HD**-0.5 * math.log2(math.e)
F32 = jnp.float32
BF16 = jnp.bfloat16


def flat(core, y, z, x):
    return ((core * 4 + y) * 2 + z % 2) * 8 + x * 2 + z // 2


def pairs(move):
    found = []
    for core in range(2):
        for y in range(4):
            for z in range(4):
                for x in range(4):
                    there = move(core, y, z, x)
                    if there is not None:
                        found.append((flat(core, y, z, x), flat(*there)))
    return sorted(found)


def out_to_heads(step):
    def move(core, y, z, x):
        half = y // 2
        return FLIP[y], (core if half == 0 else 3 - core), (z + step) % 4, x

    return pairs(move)


def back_to_tiles(step):
    return sorted((b, a) for a, b in out_to_heads(step))


def to_partner(core, y, z, x):
    return 1 - core, y, z, x


def to_outer(core, y, z, x):
    return (core, 3 - y, z, x) if core == 1 else None


def to_near(core, y, z, x):
    return core, y, z, x ^ 1


def to_far(core, y, z, x):
    return (core, y, z, 3 - x) if x in (1, 2) else None


def send(x, perm):
    return lax.ppermute(x, AXES, perm)


def turned(block):
    across = block.T
    return across[:, :HD], across[:, HD:]


def slot_cols(place, step, head):
    at = ((place[0] + step) % 4) * HEADS + head
    return pl.ds(pl.multiple_of(at * HD, HD), HD)


def pack_body(place, k_in, v_in, *outs):
    for step in range(4):
        for head in range(HEADS):
            cols = slot_cols(place, step, head)
            outs[step][head, 0] = k_in[:, cols]
            outs[step][head, 1, :HD], outs[step][head, 1, HD:] = turned(v_in[:, cols])


def pack_q_body(place, q_in, *outs):
    for step in range(4):
        for head in range(HEADS):
            outs[step][head, :HD], outs[step][head, HD:] = turned(
                q_in[:, slot_cols(place, step, head)]
            )


def placed():
    wide = lax.axis_index("wa")
    return (wide & 1) * 2 + lax.axis_index("ha"), lax.axis_index("grp"), wide >> 1, lax.axis_index("ta")


def here_body(body, *refs):
    body(placed(), *refs)


VMEM = pl.BlockSpec(memory_space=pltpu.MemorySpace.VMEM)


def local_call(body, operands, shapes, flops=0, limit=24, aliases=None):
    single = not isinstance(shapes, (list, tuple))
    listed = [shapes] if single else list(shapes)
    moved = sum(math.prod(a.shape) * a.dtype.itemsize for a in list(operands) + listed)
    return pl.pallas_call(
        functools.partial(here_body, body),
        in_specs=[VMEM] * len(operands),
        out_specs=VMEM if single else [VMEM] * len(listed),
        out_shape=shapes,
        cost_estimate=pl.CostEstimate(flops=flops, bytes_accessed=moved, transcendentals=0),
        compiler_params=pltpu.CompilerParams(vmem_limit_bytes=limit * 1024 * 1024),
        input_output_aliases=aliases or {},
    )(*operands)


def gather_body(place, *refs):
    chunks, halves, whole = refs[:4], refs[4:6], refs[6]
    for step in range(4):
        z_from = (place[0] - step + 4) % 4
        whole[z_from // 2, :, z_from % 2] = chunks[step][...]
        beside_far = z_from // 2 == place[2] % 2
        for which, chosen in ((0, jnp.logical_not(beside_far)), (1, beside_far)):

            @pl.when(chosen)
            def _():
                halves[which][:, z_from % 2] = chunks[step][...]


MIXED = jax.ShapeDtypeStruct((HEADS, 2, ROWS, 2 * TILE), F32)
PEAK = jax.ShapeDtypeStruct((HEADS, 2, 1, 2 * TILE), F32)
TURNED = jax.ShapeDtypeStruct((HEADS, 4, 2 * HD, TILE), BF16)


def spread(place, q_in, turned_q):
    for step in range(4):
        z_from = (place[0] - step + 4) % 4
        for head in range(HEADS):
            both = jnp.concatenate([q_in[step][head, :HD], q_in[step][head, HD:]], axis=1)
            scaled = both.astype(F32) * SCALE
            high = scaled.astype(BF16)
            turned_q[head, z_from, :HD] = high
            turned_q[head, z_from, HD:] = (scaled - high.astype(F32)).astype(BF16)


def loaded(tiles):
    keys = jnp.concatenate([ref[head, low, 0] for ref, head, low in tiles], axis=0)
    values = jnp.concatenate(
        [
            ref[head, low, 1, half * HD : (half + 1) * HD]
            for ref, head, low in tiles
            for half in range(2)
        ],
        axis=1,
    )
    return keys, jnp.concatenate([values, jnp.ones((ROWS - HD, values.shape[1]), BF16)], axis=0)


def queries_of(turned_q, head, side):
    return jnp.concatenate([turned_q[head, 2 * side], turned_q[head, 2 * side + 1]], axis=1)


def scored(keys, queries):
    return jnp.dot(jnp.concatenate([keys, keys], axis=1), queries, preferred_element_type=F32)


def quick(queries, tiles, level, bias=None):
    keys, values = loaded(tiles)
    scores = scored(keys, queries) - (level if bias is None else level - bias)
    return jnp.dot(values, jnp.exp2(scores).astype(BF16), preferred_element_type=F32)


def careful(turned_q, mixed, peak, head, side, ref, bias=0.0):
    def one(low, carry):
        keys, values = loaded([(ref, head, low)])
        scores = scored(keys, queries_of(turned_q, head, side)) + bias
        before = peak[head, side]
        top = jnp.maximum(before, jnp.max(scores, axis=0, keepdims=True))
        probs = jnp.exp2(scores - top).astype(BF16)
        fresh = jnp.dot(values, probs, preferred_element_type=F32)
        mixed[head, side] = mixed[head, side] * jnp.exp2(before - top) + fresh
        peak[head, side] = top
        return carry

    lax.fori_loop(0, 2, one, 0)


def both_lows(head, *refs):
    return [(ref, head, low) for ref in refs for low in range(2)]


def within(sums):
    return jnp.max(sums) < LIMIT


def redo(turned_q, mixed, peak, shares, sides, biases):
    def one(head, carry):
        for part in range(2):
            for ref in shares[part]:
                careful(turned_q, mixed, peak, head, sides[part], ref, 0.0 if part == 0 else biases[1])
        return carry

    lax.fori_loop(0, HEADS, one, 0)


def redo_alike(turned_q, mixed, peak, refs):
    def one(at, carry):
        for ref in refs:
            careful(turned_q, mixed, peak, at // 2, at % 2, ref)
        return carry

    lax.fori_loop(0, 2 * HEADS, one, 0)


def copied(source, target):
    def one(head, carry):
        target[head] = source[head]
        return carry

    lax.fori_loop(0, HEADS, one, 0)


def larger(one, two):
    return two if one is None else jnp.maximum(one, two)


def first_body(place, *refs):
    own, inner, q_in, (turned_q, mixed, peak) = refs[:2], refs[2], refs[3:7], refs[7:]
    inner = (inner.at[0], inner.at[1])
    spread(place, q_in, turned_q)

    def one(head, worst):
        for side in range(2):
            queries = queries_of(turned_q, head, side)
            level = jnp.max(scored(own[0][head, 0, 0, :HD], queries), axis=0, keepdims=True)
            peak[head, side] = level
            fresh = quick(queries, both_lows(head, *own), level) + quick(
                queries, both_lows(head, *inner), level
            )
            mixed[head, side] = fresh
            worst = jnp.maximum(worst, fresh[HD : HD + 8])
        return worst

    worst = jnp.zeros((8, 2 * TILE), F32)
    for head in range(HEADS):
        worst = one(head, worst)

    @pl.when(jnp.logical_not(within(worst)))
    def _():
        mixed[...] = jnp.zeros_like(mixed)
        redo_alike(turned_q, mixed, peak, (*own, *inner))


def more(turned_q, mixed_in, mixed, peak, shares, sides=(0, 1), biases=(None, None)):
    worst = None
    for head in range(HEADS):
        for part in range(2):
            side = sides[part]
            fresh = mixed_in[head, side] + quick(
                queries_of(turned_q, head, side),
                both_lows(head, *shares[part]),
                peak[head, side],
                biases[part],
            )
            mixed[head, side] = fresh
            worst = larger(worst, fresh[HD : HD + 8])
    return within(worst)


def edge_sides(place):
    far_side = place[2] % 2
    missing = jnp.logical_or(place[2] == 0, place[2] == 3)
    return (1 - far_side, far_side), (None, jnp.where(missing, -1e30, 0.0).astype(F32))


def second_body(place, *refs):
    outer, (turned_q, mixed_in, _, mixed, peak) = refs[:2], refs[2:]

    @pl.when(place[1] == 0)
    def _():
        copied(mixed_in, mixed)

    @pl.when(place[1] == 1)
    def _():
        good = more(turned_q, mixed_in, mixed, peak, (outer, outer))

        @pl.when(jnp.logical_not(good))
        def _():
            copied(mixed_in, mixed)
            redo_alike(turned_q, mixed, peak, outer)


def third_body(place, *refs):
    near, far, turned_q, mixed_in, _, mixed, peak = refs
    sides, biases = edge_sides(place)
    shares = (near,), (far,)
    good = more(turned_q, mixed_in, mixed, peak, shares, sides, biases)

    @pl.when(jnp.logical_not(good))
    def _():
        copied(mixed_in, mixed)
        redo(turned_q, mixed, peak, shares, sides, biases)


def last_body(place, *refs):
    outs, (peak, mixed, done) = refs[5:9], refs[9:]

    @pl.when(place[1] == 1)
    def _():
        third_body(place, *refs[:5], mixed, peak)

    @pl.when(place[1] == 0)
    def _():
        copied(refs[3], mixed)

    for head in range(HEADS):
        for side in range(2):
            inverse = 1.0 / mixed[head, side, HD : HD + 1]
            result = (mixed[head, side, :HD] * inverse).astype(BF16).T
            for low in range(2):
                done[2 * side + low, head] = result[low * TILE : (low + 1) * TILE]

    for step in range(4):
        z_from = (place[0] - step + 4) % 4
        for head in range(HEADS):
            outs[step][:, head * HD : (head + 1) * HD] = done[z_from, head]


def last(operands, flops):
    out = jax.ShapeDtypeStruct((TILE, HEADS * HD), BF16)
    return pl.pallas_call(
        functools.partial(here_body, last_body),
        in_specs=[VMEM] * len(operands),
        out_specs=[VMEM] * 5,
        out_shape=[out] * 4 + [PEAK],
        scratch_shapes=[pltpu.VMEM(MIXED.shape, F32), pltpu.VMEM((4, HEADS, TILE, HD), BF16)],
        input_output_aliases={4: 4},
        cost_estimate=pl.CostEstimate(flops=flops, bytes_accessed=1 << 20, transcendentals=0),
        compiler_params=pltpu.CompilerParams(vmem_limit_bytes=24 * 1024 * 1024),
        name="last",
    )(*operands)[:4]


def join_body(place, *refs):
    chunks, joined = refs[:4], refs[4]
    for step in range(4):
        for head in range(HEADS):
            joined[:, slot_cols(place, step, head)] = chunks[step][:, head * HD : (head + 1) * HD]


def own_cols(core, width):
    return pl.ds(pl.multiple_of(core * width, width), width)


def home_body(place, joined, weight, out):
    cols = own_cols(place[1], out.shape[1])
    out[...] = jnp.dot(joined[...], weight[:, cols], preferred_element_type=F32)


def cut_body(place, weight, out):
    out[...] = weight[:, own_cols(1 - place[1], out.shape[1])]


def close_body(here, joined, weight, gate, out, held, sent):
    cols = held.shape[1] // 3
    copies = []
    for part in range(3):
        block = slice(part * cols, (part + 1) * cols)
        there = jnp.dot(joined[...], weight[:, block], preferred_element_type=F32)
        total = here[:, block] + there
        held[:, block] = (gate[:, block].astype(F32) * total).astype(BF16)
        copy = pltpu.make_async_copy(
            held.at[:, pl.ds(part * cols, cols)], out.at[:, pl.ds(part * cols, cols)], sent.at[part]
        )
        copy.start()
        copies.append(copy)
    for copy in copies:
        copy.wait()


def close(here, joined, weight, gate):
    features = weight.shape[0]
    return pl.pallas_call(
        close_body,
        in_specs=[VMEM] * 4,
        out_specs=pl.BlockSpec(memory_space=pltpu.MemorySpace.HBM),
        out_shape=jax.ShapeDtypeStruct((TILE, features), BF16),
        scratch_shapes=[pltpu.VMEM((TILE, features), BF16), pltpu.SemaphoreType.DMA((3,))],
        cost_estimate=pl.CostEstimate(
            flops=2 * TILE * features * features, bytes_accessed=1 << 20, transcendentals=0
        ),
        compiler_params=pltpu.CompilerParams(vmem_limit_bytes=24 * 1024 * 1024),
        name="close",
    )(here, joined, weight, gate)


def shards(query_tiles, key_tiles, value_tiles, out_weight, gate):
    features = query_tiles.shape[4]
    q, k, v = (a.reshape(TILE, features) for a in (query_tiles, key_tiles, value_tiles))
    partner, outer_pairs = pairs(to_partner), pairs(to_outer)
    near_pairs, far_pairs = pairs(to_near), pairs(to_far)
    upper = flat(1, 0, 0, 0)
    near_upper, far_upper = ([p for p in perm if p[0] >= upper] for perm in (near_pairs, far_pairs))
    flops_of = lambda tiles: HEADS * 4 * TILE * tiles * TILE * 6 * HD

    kv_shape = jax.ShapeDtypeStruct((HEADS, 2, TILE, HD), BF16)
    kv_sent = local_call(pack_body, [k, v], [kv_shape] * 4)
    kv = [send(kv_sent[s], out_to_heads(s)) for s in range(4)]
    q_shape = jax.ShapeDtypeStruct((HEADS, TILE, HD), BF16)
    q_sent = local_call(pack_q_body, [q], [q_shape] * 4)
    queries = [send(q_sent[s], out_to_heads(s)) for s in range(4)]
    weight_away = local_call(
        cut_body, [out_weight], jax.ShapeDtypeStruct((features, features), BF16)
    )
    weight_other = send(weight_away, partner)
    half = (HEADS, 2, 2, TILE, HD)
    *own, whole = local_call(
        gather_body, kv,
        [jax.ShapeDtypeStruct(half, BF16)] * 2 + [jax.ShapeDtypeStruct((2, *half), BF16)],
    )
    outer = [send(own[i], outer_pairs) for i in range(2)]
    inner = send(whole, partner)
    near, far = send(own[0], near_pairs), send(own[1], far_pairs)
    state = local_call(first_body, [*own, inner, *queries], [TURNED, MIXED, PEAK], flops_of(8))
    turned_q, mixed, peak = state
    near_outer = send(outer[0], near_upper)
    far_outer = send(outer[1], far_upper)
    mixed, peak = local_call(
        second_body, [*outer, turned_q, mixed, peak], [MIXED, PEAK],
        flops_of(4), aliases={4: 1},
    )
    near_inner, far_inner = send(near, partner), send(far, partner)
    mixed, peak = local_call(
        third_body, [near, far, turned_q, mixed, peak],
        [MIXED, PEAK], flops_of(2), aliases={4: 1},
    )
    mixed, peak = local_call(
        third_body, [near_inner, far_inner, turned_q, mixed, peak],
        [MIXED, PEAK], flops_of(2), aliases={4: 1},
    )
    outs = last([near_outer, far_outer, turned_q, mixed, peak], flops_of(2))
    chunks = [send(outs[s], back_to_tiles(s)) for s in range(4)]
    joined = local_call(join_body, chunks, jax.ShapeDtypeStruct((TILE, features), BF16))
    arrived = send(joined, partner)
    flops = 2 * TILE * features * features
    here = local_call(
        home_body, [joined, out_weight], jax.ShapeDtypeStruct((TILE, features), F32), flops
    )
    branch = close(here, arrived, weight_other, gate.reshape(1, -1))
    return branch.reshape(1, 1, 1, TILE, features)


def solution(mesh):
    spec = P("ta", "ha", "wa", None, "grp")

    return jax.shard_map(
        shards,
        mesh=mesh,
        in_specs=(spec, spec, spec, P("grp", None), P("grp")),
        out_specs=spec,
        check_vma=False,
    )
```
